256 devices in a mesh: expert: 32 (over y, x, core), tensor: 8 (over z).
Axes of the slice: x: 4, y: 4, z: 8, core: 2. Of those that a mesh axis runs over, the one named last changes fastest.
Arguments:
- tokens: bfloat16 [32768, 1024], P(('expert', 'tensor')), may hold values from -6 to 6
- grad_out: bfloat16 [32768, 1024], P(('expert', 'tensor')), may hold values from -6 to 6
- expert_ids: int32 [32768, 2], P(('expert', 'tensor')), may hold values from 0 to 31, all different within a row; in each aligned block of 128 rows (0 to 127, 128 to 255, ...) at most 12 rows name the same one
- probs: float32 [32768, 2], P(('expert', 'tensor')), may hold values from 0.2 to 1
- w_gate: bfloat16 [32, 1024, 2048], P('expert', None, 'tensor'), may hold values from -0.1875 to 0.1875
- w_up: bfloat16 [32, 1024, 2048], P('expert', None, 'tensor'), may hold values from -0.1875 to 0.1875
- w_down: bfloat16 [32, 2048, 1024], P('expert', 'tensor'), may hold values from -0.125 to 0.125
Outputs:
- d_tokens: bfloat16 [32768, 1024], P(('expert', 'tensor'))
- d_probs: float32 [32768, 2], P(('expert', 'tensor'))
- d_w_gate: float32 [32, 1024, 2048], P('expert', None, 'tensor')
- d_w_up: float32 [32, 1024, 2048], P('expert', None, 'tensor')
- d_w_down: float32 [32, 2048, 1024], P('expert', 'tensor')
The draws below stay inside these ranges and needn't reach their ends.
Inputs may be any that keep to these rules, and one draw needn't show every extreme that they name: `expert_ids`: the two experts of a token differ. In each aligned block of 128 rows (the rows of one device) no expert is named more than 12 times, and in some block one expert is named exactly 12 times.
All inputs are finite; a program needn't handle non-finite values.
Results may differ from the reference program's by a relative error of at most 0.015.
Values may be sent and summed in bfloat16 or wider, within the bound.
A program may use at most 128 MiB of HBM per device.

```python
import math
import jax
import jax.numpy as jnp
import numpy as np
from jax import lax

D = 1024
FF = 2048
TOP = 2
TOK_DEV = 128
EXPERTS = 32
CAP = 12
ROWS = 3072
TOKENS = 32768
N_TENSOR = 8


def block_levels(own_key, dims, split, smallest, top_value):
    def one(dim, parts):
        draws = jax.random.uniform(jax.random.fold_in(jax.random.fold_in(own_key, 6), dim), (parts,), jnp.float32, smallest / len(split), top_value / len(split))
        return jnp.repeat(jnp.exp(draws), dims[dim] // parts).reshape((-1,) + (1,) * (len(dims) - dim - 1))

    factor_of = one(*split[0])
    for cut in split[1:]:
        factor_of = factor_of * one(*cut)
    return factor_of


def shared_out(own_key, own, number, rows, amount, top, reach, skew):
    order = jax.random.permutation(own_key, amount)
    heavy_load, common = shares(amount, rows * top, reach, skew, True), shares(amount, rows * top, reach, skew, False)
    places = jnp.arange(amount)

    def named(lengths, rotation):
        used = int((lengths > 0).sum())
        fixed = max(1, used // 4)
        shifted = fixed + (places - fixed + rotation * (used - fixed)) % max(1, amount - fixed)
        return jnp.zeros((amount,), jnp.int32).at[order[jnp.where(places < fixed, places, shifted)]].set(jnp.asarray(lengths, jnp.int32))

    lengths = jnp.where(number % 4 == 0, named(heavy_load, number // 4), named(common, number - number // 4 - 1))
    mixed = jax.random.permutation(jax.random.fold_in(own, 3), amount)
    giver, sink = mixed[0:amount // 2 * 2:2], mixed[1:amount // 2 * 2:2]
    room = jnp.minimum(lengths[giver] - 1, reach - lengths[sink]) // 2
    room = jnp.where((giver == order[0]) | (sink == order[0]) | (lengths[sink] == 0), 0, jnp.maximum(room, 0))
    shifted = jax.random.randint(jax.random.fold_in(own, 4), (amount // 2,), 0, 1 << 20) % (room + 1)
    lengths = lengths.at[giver].add(-shifted).at[sink].add(shifted)
    items = jnp.searchsorted(jnp.cumsum(lengths), jnp.arange(rows * top), side="right").astype(jnp.int32)
    grid = items.reshape(top, rows).T
    grid = grid[jax.random.permutation(jax.random.fold_in(own, 1), rows)]
    rotation = jax.random.randint(jax.random.fold_in(own, 2), (rows, 1), 0, top)
    return jnp.take_along_axis(grid, (jnp.arange(top)[None, :] + rotation) % top, axis=1)


def shares(amount, total, bound, lean, full):
    portions = [(1 << 20) // math.isqrt(grade ** lean) + 1 for grade in range(1, amount + 1)]
    largest = bound if full else min(bound, max(-(-total // amount), total * portions[0] // sum(portions)))
    least = 1 if total - largest >= amount - 1 else 0
    given, rest = [largest] + [least] * (amount - 1), total - largest - least * (amount - 1)
    while rest > 0:
        candidates = [i for i in range(1, amount) if given[i] < largest] or [i for i in range(1, amount) if given[i] < bound]
        mass, left = sum([portions[i] for i in candidates]), rest
        for i in candidates:
            more = min(bound - given[i], max(1, left * portions[i] // mass), rest)
            given[i] = given[i] + more
            rest = rest - more
    return np.array(given)


def centred(own_key, extent, scale, most, pieces=(), kind=jnp.bfloat16):
    result = jax.random.normal(own_key, extent, jnp.float32) * scale
    if len(pieces) > 0:
        result = block_levels(own_key, extent, pieces, -0.22, 0.18) * result
    return jnp.clip(result, min=-most, max=most).astype(kind)


def setup_inputs(seed: int = 0) -> dict:
    seeds = jax.random.split(jax.random.key(seed), 8)
    tokens = centred(seeds[0], (TOKENS, D), 1.0, 6.0, ((0, 256),))
    grad_out = centred(seeds[1], (TOKENS, D), 1.0, 6.0, ((0, 256),))
    expert_ids_keys = jax.random.split(jax.random.fold_in(seeds[2], 1), TOKENS // TOK_DEV)
    expert_ids_turns = jax.random.permutation(jax.random.fold_in(seeds[2], 3), TOKENS // TOK_DEV)
    expert_ids = jax.vmap(lambda own, number: shared_out(jax.random.fold_in(seeds[2], 2), own, number, TOK_DEV, EXPERTS, TOP, CAP, 2))(expert_ids_keys, expert_ids_turns).reshape((TOKENS, TOP))
    probs = jnp.clip(0.2 + 0.8 * jax.random.uniform(seeds[3], (TOKENS, TOP), jnp.float32) ** block_levels(seeds[3], (TOKENS, TOP), ((0, 256),), -0.2, 0.2), 0.2, 1.0)
    w_gate = centred(seeds[4], (EXPERTS, D, FF), D ** -0.5, 0.1875, ((0, 32), (2, 8)))
    w_up = centred(seeds[5], (EXPERTS, D, FF), D ** -0.5, 0.1875, ((0, 32), (2, 8)))
    w_down = centred(seeds[6], (EXPERTS, FF, D), FF ** -0.5, 0.125, ((0, 32), (1, 8)))
    return dict(tokens=tokens, grad_out=grad_out, expert_ids=expert_ids, probs=probs, w_gate=w_gate, w_up=w_up, w_down=w_down)


def reference(tokens, grad_out, expert_ids, probs, w_gate, w_up, w_down):
    assigns = TOKENS * TOP
    span_units = FF // N_TENSOR
    flat_ids = expert_ids.reshape(-1).astype(jnp.int32)
    order = jnp.argsort(flat_ids, stable=True).astype(jnp.int32)
    counts = jnp.sum((flat_ids[:, None] == jnp.arange(EXPERTS, dtype=jnp.int32)[None, :]).astype(jnp.int32), axis=0)
    starts = (jnp.cumsum(counts) - counts).astype(jnp.int32)
    order_pad = jnp.concatenate([order, jnp.full((ROWS,), assigns, jnp.int32)])
    token_pad = jnp.concatenate([tokens, jnp.zeros((1, D), tokens.dtype)])
    grad_pad = jnp.concatenate([grad_out, jnp.zeros((1, D), grad_out.dtype)])
    prob_pad = jnp.concatenate([probs.reshape(-1).astype(jnp.bfloat16), jnp.zeros((1,), jnp.bfloat16)])

    def one_expert(expert):
        picked = lax.dynamic_slice(order_pad, (starts[expert],), (ROWS,))
        live = jnp.arange(ROWS, dtype=jnp.int32) < counts[expert]
        picked = jnp.where(live, picked, jnp.int32(assigns)).astype(jnp.int32)
        rows_in = token_pad[picked // TOP]
        rows_grad = grad_pad[picked // TOP]
        weight = prob_pad[picked].astype(jnp.float32)[:, None]
        gate_mat = w_gate[expert]
        up_mat = w_up[expert]
        down_mat = w_down[expert]
        gate_pre = jnp.dot(rows_in, gate_mat, preferred_element_type=jnp.float32)
        up_pre = jnp.dot(rows_in, up_mat, preferred_element_type=jnp.float32)
        sigmoid = jax.nn.sigmoid(gate_pre)
        swished = gate_pre * sigmoid
        hidden = swished * up_pre
        hidden_w = (weight * hidden).astype(jnp.bfloat16)
        act_raw = jnp.dot(rows_grad, down_mat.T, preferred_element_type=jnp.float32)
        act_grad = weight * act_raw
        gate_grad = (act_grad * up_pre * sigmoid * (1.0 + gate_pre * (1.0 - sigmoid))).astype(jnp.bfloat16)
        up_grad = (act_grad * swished).astype(jnp.bfloat16)
        down_wgrad = jnp.dot(hidden_w.T, rows_grad, preferred_element_type=jnp.float32)
        gate_wgrad = jnp.dot(rows_in.T, gate_grad, preferred_element_type=jnp.float32)
        up_wgrad = jnp.dot(rows_in.T, up_grad, preferred_element_type=jnp.float32)
        input_grad = jnp.zeros((ROWS, D), jnp.float32)
        prob_grad = jnp.zeros((ROWS,), jnp.float32)
        for section in range(N_TENSOR):
            offset = section * span_units
            upper = offset + span_units
            partial_value = jnp.dot(gate_grad[:, offset:upper], gate_mat[:, offset:upper].T, preferred_element_type=jnp.float32)
            partial_value = partial_value + jnp.dot(up_grad[:, offset:upper], up_mat[:, offset:upper].T, preferred_element_type=jnp.float32)
            partial_value = lax.optimization_barrier(partial_value.astype(jnp.bfloat16))
            input_grad = input_grad + partial_value.astype(jnp.float32)
            prob_piece = jnp.sum(hidden[:, offset:upper] * act_raw[:, offset:upper], axis=1)
            prob_piece = lax.optimization_barrier(prob_piece.astype(jnp.bfloat16))
            prob_grad = prob_grad + prob_piece.astype(jnp.float32)
        return gate_wgrad, up_wgrad, down_wgrad, input_grad, prob_grad, picked

    results = lax.map(one_expert, jnp.arange(EXPERTS, dtype=jnp.int32))
    gate_all, up_all, down_all, input_all, prob_all, picked_all = results
    where_to = picked_all.reshape(-1)
    input_assign = jnp.zeros((assigns + 1, D), jnp.float32).at[where_to].add(input_all.reshape(-1, D))[:assigns]
    prob_assign = jnp.zeros((assigns + 1,), jnp.float32).at[where_to].add(prob_all.reshape(-1))[:assigns]
    d_tokens = jnp.sum(input_assign.reshape(TOKENS, TOP, D), axis=1).astype(jnp.bfloat16)
    d_probs = prob_assign.reshape(TOKENS, TOP)
    return d_tokens, d_probs, gate_all, up_all, down_all
```

```python
import jax
import jax.numpy as jnp
from jax import lax
from jax.sharding import PartitionSpec as P

F32 = jnp.float32
BF16 = jnp.bfloat16


def dot(a, b, ca, cb):
    return lax.dot_general(a, b, (((ca,), (cb,)), ((), ())), preferred_element_type=F32)


def slot_masks(ids, experts, capacity):
    rows = ids.shape[1]
    lane = jnp.arange(experts, dtype=jnp.int32)[:, None]
    hot = [(lane == ids[j][None, :]).astype(BF16) for j in range(ids.shape[0])]
    order = jnp.arange(rows, dtype=jnp.int32)
    before = (order[:, None] < order[None, :]).astype(BF16)
    earlier = dot(hot[0] + hot[1], before, 1, 0)
    slots = jnp.arange(experts * capacity, dtype=jnp.int32)[:, None]
    masks = []
    for j in range(ids.shape[0]):
        place = jnp.sum(hot[j].astype(F32) * earlier, axis=0).astype(jnp.int32)
        masks.append(slots == (ids[j] * capacity + place)[None, :])
    return masks


def expert_backward(rows_in, rows_grad, gate_mat, up_mat, down_mat):
    gate_pre = dot(rows_in, gate_mat, 1, 0)
    up_pre = dot(rows_in, up_mat, 1, 0)
    sigmoid = jax.nn.sigmoid(gate_pre)
    swished = gate_pre * sigmoid
    hidden = swished * up_pre
    act = dot(rows_grad, down_mat, 1, 1)
    prob_part = jnp.sum(hidden * act, axis=1)
    gate_grad = (act * up_pre * sigmoid * (1.0 + gate_pre * (1.0 - sigmoid))).astype(BF16)
    up_grad = (act * swished).astype(BF16)
    input_part = dot(gate_grad, gate_mat, 1, 1) + dot(up_grad, up_mat, 1, 1)
    down_wgrad = dot(hidden.astype(BF16), rows_grad, 0, 0)
    gate_wgrad = dot(rows_in, gate_grad, 0, 0)
    up_wgrad = dot(rows_in, up_grad, 0, 0)
    return input_part.astype(BF16), prob_part, gate_wgrad, up_wgrad, down_wgrad


def per_device(tokens, grad_out, expert_ids, probs, w_gate, w_up, w_down):
    experts = lax.axis_size("expert") * w_gate.shape[0]
    own_rows = tokens.shape[0]
    picks = expert_ids.shape[1]
    capacity = max(2, 3 * own_rows * picks // (2 * experts))
    masks = slot_masks(expert_ids.T, experts, capacity)
    prob_b = probs.astype(BF16).T
    pick_of = sum(m.astype(BF16) for m in masks)
    weight_of = sum(jnp.where(masks[j], prob_b[j][None, :], 0) for j in range(picks))
    send_in = dot(pick_of, tokens, 1, 0).astype(BF16)
    send_grad = dot(weight_of, grad_out, 1, 0).astype(BF16)

    def exchange(a):
        return lax.all_to_all(a, "expert", split_axis=0, concat_axis=0, tiled=True)

    rows_in = lax.all_gather(exchange(send_in), "tensor", axis=0, tiled=True)
    rows_grad = lax.all_gather(exchange(send_grad), "tensor", axis=0, tiled=True)
    input_part, prob_part, gate_wgrad, up_wgrad, down_wgrad = expert_backward(
        rows_in, rows_grad, w_gate[0], w_up[0], w_down[0]
    )
    back_prob = exchange(lax.psum_scatter(prob_part, "tensor", scatter_dimension=0, tiled=True))
    back_in = exchange(lax.psum_scatter(input_part, "tensor", scatter_dimension=0, tiled=True))
    d_tokens = dot(pick_of, back_in, 0, 0).astype(BF16)
    d_probs = jnp.stack(
        [jnp.sum(jnp.where(m, back_prob[:, None], 0.0), axis=0) for m in masks], axis=1
    )
    d_probs = d_probs / prob_b.T.astype(F32)
    return (d_tokens, d_probs, gate_wgrad[None], up_wgrad[None], down_wgrad[None])


def solution(mesh):
    rows = P(("expert", "tensor"), None)
    cols = P("expert", None, "tensor")
    down = P("expert", "tensor", None)
    return jax.shard_map(
        per_device,
        mesh=mesh,
        in_specs=(rows, rows, rows, rows, cols, cols, down),
        out_specs=(rows, rows, cols, cols, down),
        check_vma=False,
    )
```
